32 devices in a mesh: rep: 4 (over z), tp: 8 (over y, x, core).
Axes of the slice: x: 2, y: 2, z: 4, core: 2. Of those that a mesh axis runs over, the one named last changes fastest.
Arguments:
- attn: bfloat16 [3072, 4096], P('rep', 'tp'), parts along dimension 0, may hold values from -6 to 6
- output_weight: bfloat16 [4096, 8192], P(None, 'tp'), may hold values from -0.09375 to 0.09375
- adapter_down_weight: bfloat16 [8, 64, 4096], P('tp'), may hold values from -0.09375 to 0.09375
- adapter_up_weight: bfloat16 [8, 64, 8192], P('tp'), may hold values from -0.75 to 0.75
- block_adapter_index: int32 [24], P('rep'), parts along dimension 0, may hold values from 0 to 7
- adapter_page_table: int32 [8], replicated, may hold values from 0 to 7, each once
Outputs:
- projected: bfloat16 [3072, 8192], P('rep', 'tp'), parts along dimension 0
The draws below stay inside these ranges and needn't reach their ends.
There are 4 independent parts, one for each index of `rep`. The reference program is written for one: setup_inputs(seed, part) draws one part's arguments, and reference() takes and returns one part's arrays. A program takes and returns all parts, laid end to end along the dimension named above; an argument that names none is the same for every part. Nothing has to cross between parts.
Inputs may be any that keep to these rules, and one draw needn't show every extreme that they name: adapter_page_table is a permutation; adapter a is stored on tp device adapter_page_table[a] (each device holds exactly one adapter), and row adapter_page_table[a] of adapter_down_weight and adapter_up_weight holds it. `block_adapter_index`: the adapter used by all 128 tokens of a block.
All inputs are finite; a program needn't handle non-finite values.
Results may differ from the reference program's by a relative error of at most 0.0046.
Values may be sent and summed in bfloat16 or wider, within the bound.
A program may use at most 64 MiB of HBM per device.

```python
import jax
import jax.numpy as jnp
from jax import lax

MODEL_WIDTH = 8192
ADAPTER_RANK = 64
BLOCK = 128
TOKENS = 768
ATTN_FEATURES = 4096
ADAPTER_COUNT = 8
BLOCKS = 6


def place_ends(array, own_key, least, high):
    index_at = [jax.random.randint(jax.random.fold_in(own_key, axis), (), 0, length) for axis, length in enumerate(array.shape)]
    longest = array.shape.index(max(array.shape))
    neighbour = index_at[:longest] + [(index_at[longest] + 1) % array.shape[longest]] + index_at[longest + 1:]
    return array.at[tuple(index_at)].set(least).at[tuple(neighbour)].set(high)


def levels(own_key, extent, shards, smallest, high):
    gain, own = 1.0, jax.random.fold_in(own_key, 6)
    for position, blocks in shards:
        steps = jnp.exp(jax.random.uniform(jax.random.fold_in(own, position), (blocks,), jnp.float32, smallest / len(shards), high / len(shards)))
        gain = gain * jnp.repeat(steps, extent[position] // blocks).reshape([-1 if axis == position else 1 for axis in range(len(extent))])
    return gain


def noise(own_key, shape, deviation, reach, cuts=(), held_as=jnp.bfloat16):
    drawn = jax.random.normal(own_key, shape, jnp.float32) * deviation
    if len(cuts) > 0:
        drawn = levels(own_key, shape, cuts, -0.22, 0.18) * drawn
    return jnp.clip(drawn, min=-reach, max=reach).astype(held_as)


def setup_inputs(seed: int = 0, part: int = 0) -> dict:
    key_list = jax.random.split(jax.random.key(seed), 7)
    own_keys = jax.random.split(jax.random.fold_in(key_list[6], part), 7)
    attn = noise(own_keys[0], (TOKENS, ATTN_FEATURES), 1.0, 6.0, ((1, 8),))
    output_weight = noise(key_list[1], (ATTN_FEATURES, MODEL_WIDTH), ATTN_FEATURES ** -0.5, 0.09375, ((1, 8),))
    adapter_down_weight = noise(key_list[2], (ADAPTER_COUNT, ADAPTER_RANK, ATTN_FEATURES), ATTN_FEATURES ** -0.5, 0.09375, ((0, 8),))
    adapter_up_weight = noise(key_list[3], (ADAPTER_COUNT, ADAPTER_RANK, MODEL_WIDTH), ADAPTER_RANK ** -0.5, 0.75, ((0, 8),))
    block_adapter_index = place_ends(jax.random.randint(own_keys[4], (BLOCKS,), 0, ADAPTER_COUNT), jax.random.fold_in(own_keys[4], 1), 0, ADAPTER_COUNT - 1).astype(jnp.int32)
    adapter_page_table = jax.random.permutation(key_list[5], ADAPTER_COUNT).astype(jnp.int32)
    return {"attn": attn, "output_weight": output_weight, "adapter_down_weight": adapter_down_weight, "adapter_up_weight": adapter_up_weight, "block_adapter_index": block_adapter_index, "adapter_page_table": adapter_page_table}


adapter_scale = 2.0


def reference(attn, output_weight, adapter_down_weight, adapter_up_weight, block_adapter_index, adapter_page_table):
    block_page_index = adapter_page_table[block_adapter_index].astype(jnp.int32)
    base_output = jnp.dot(attn, output_weight, preferred_element_type=jnp.float32)
    row_blocks = attn.reshape(BLOCKS, BLOCK, ATTN_FEATURES).astype(jnp.float32)
    down_block_rows = adapter_down_weight[block_page_index].astype(jnp.float32)
    shrunk = jnp.einsum("btf,brf->brt", row_blocks, down_block_rows, precision=lax.Precision.HIGHEST)
    shrunk_low = lax.optimization_barrier(shrunk.astype(jnp.bfloat16))
    up_block_rows = adapter_up_weight[block_page_index].astype(jnp.float32)
    adapter_output = jnp.einsum("brt,brc->btc", shrunk_low.astype(jnp.float32), up_block_rows, precision=lax.Precision.HIGHEST)
    adapter_output = adapter_output.reshape(TOKENS, MODEL_WIDTH)
    return (base_output + adapter_scale * adapter_output).astype(jnp.bfloat16)
```

```python
import functools

import jax
import jax.numpy as jnp
from jax import lax
from jax.experimental import pallas as pl
from jax.experimental.pallas import tpu as pltpu
from jax.sharding import PartitionSpec as P

adapter_scale = 2.0
MESH = pl.DeviceIdType.MESH


def plain_shards(
    attn,
    output_weight,
    adapter_down_weight,
    adapter_up_weight,
    block_adapter_index,
    adapter_page_table,
):
    tokens = attn.shape[0]
    blocks = block_adapter_index.shape[0]
    block_rows = tokens // blocks
    page_slot_count = adapter_down_weight.shape[0]
    width_out = output_weight.shape[1]
    position = lax.axis_index("tp")
    block_page_index = adapter_page_table[block_adapter_index]
    up_weight_columns = lax.all_to_all(
        adapter_up_weight, "tp", split_axis=2, concat_axis=0, tiled=True
    )
    block_up = up_weight_columns[block_page_index]
    gathered = lax.all_gather(attn, "tp", axis=1, tiled=True)
    base_output = jnp.dot(gathered, output_weight, preferred_element_type=jnp.float32)
    row_blocks = gathered.reshape(blocks, block_rows, gathered.shape[1])
    side_sum = jnp.einsum(
        "btf,srf->bsrt", row_blocks, adapter_down_weight, preferred_element_type=jnp.float32
    )
    own_pages = position * page_slot_count + jnp.arange(page_slot_count, dtype=jnp.int32)
    owned = (block_page_index[:, None] == own_pages[None, :]).astype(jnp.float32)
    local_term = jnp.sum(owned[:, :, None, None] * side_sum, axis=1)
    shrunk = lax.psum(local_term.astype(jnp.bfloat16), "tp")
    adapter_output = jnp.einsum(
        "brt,brc->btc", shrunk, block_up, preferred_element_type=jnp.float32
    )
    adapter_output = adapter_output.reshape(tokens, width_out)
    return (base_output + adapter_scale * adapter_output).astype(jnp.bfloat16)


depth = 4
split = 2
z_parts = 2


def link_orders(chunks):
    x_order, y_order = [(False, 1), (False, 0), (False, 3)], [(False, 0), (False, 1), (False, 2)]
    for s in range(chunks // 2):
        x_order.append((True, 2 * s))
        y_order.append((True, 2 * s + 1))
        for order, b in ((x_order, 2 * s + 2), (x_order, 2 * s + 5), (y_order, 2 * s + 3), (y_order, 2 * s + 4)):
            if b < chunks:
                order.append((False, b))
    return x_order, y_order


def semaphore_counts(blocks, reps):
    sends = 9 + 5 + 2 * z_parts * (reps - 1)
    receives = 3 * blocks * split // 2 + 2 * blocks + 8 + 2 * z_parts * (reps - 1)
    return sends, receives


def kernel(
    n,
    reps,
    index_ref,
    table_ref,
    attn_ref,
    weight_ref,
    down_ref,
    up_ref,
    out_ref,
    a_all,
    w_all,
    acc,
    dn_own,
    up_own,
    dn_all,
    up_all,
    part,
    half_in,
    chip_part,
    x_out,
    x_in,
    y_out,
    y_in,
    sum_all,
    send_sem,
    recv_sem,
    local_sem,
    far_sem,
):
    blocks = index_ref.shape[0]
    chunks = blocks * split
    rows = a_all.shape[1] // blocks
    chunk_rows = rows // split
    rank = dn_all.shape[1]
    f_own = a_all.shape[2]
    c_own = up_all.shape[2]
    width = acc.shape[1]
    me = lax.axis_index("tp")
    z = lax.axis_index("rep")
    core = lax.rem(me, 2)
    x_at = lax.rem(me // 2, 2)
    y_at = me // 4
    mate = me + 1 - 2 * core
    xn = me + 2 - 4 * x_at
    yn = me + 4 - 8 * y_at
    dg = xn + 4 - 8 * y_at
    zp = z + 1 - 2 * lax.rem(z, 2)

    def mate_of(d):
        return d + 1 - 2 * core

    counts = {"send": 0, "recv": 0, "local": 0}

    def take(kind, many=1):
        k = counts[kind]
        counts[kind] += many
        return k

    def remote(src, dst, axis, target, s, r):
        return pltpu.make_async_remote_copy(
            src_ref=src,
            dst_ref=dst,
            send_sem=send_sem.at[s],
            recv_sem=recv_sem.at[r],
            device_id={axis: target},
            device_id_type=MESH,
        )

    def drain(sem, ref):
        pltpu.make_async_copy(ref, ref, sem).wait()

    singles = []

    def single(src, dst, axis, target):
        copy = remote(src, dst, axis, target, take("send"), take("recv"))
        copy.start()
        singles.append(copy)
        return copy

    def local(src, dst, k=None):
        copy = pltpu.make_async_copy(src, dst, local_sem.at[take("local") if k is None else k])
        copy.start()
        return copy

    quarter = rank // reps
    pair_rank = rank // 2

    def quarter_of(at):
        return pl.ds(pl.multiple_of(at * quarter, quarter), quarter)

    up_rows = quarter_of(z)
    dn_rows = pl.ds(pl.multiple_of(lax.rem(z, 2) * pair_rank, pair_rank), pair_rank)
    own_f = pl.ds(pl.multiple_of(me * f_own, f_own), f_own)
    own_c = pl.ds(pl.multiple_of(me * c_own, c_own), c_own)

    dn_stage = local(down_ref.at[0, dn_rows, :], dn_own)
    up_stage = local(up_ref.at[0, up_rows, :], up_own)
    own_load = local(attn_ref, a_all.at[me])
    own_dn = local(down_ref.at[0, dn_rows, own_f], dn_all.at[me, dn_rows, :])
    own_up = local(up_ref.at[0, up_rows, own_c], up_all.at[me, up_rows, :])

    barrier = pltpu.get_barrier_semaphore()
    near = (xn, yn, mate_of(xn), mate_of(yn), mate)
    for d in near:
        pl.semaphore_signal(barrier, inc=1, device_id={"tp": d}, device_id_type=MESH)

    @pl.when(z + 1 < reps)
    def _():
        pl.semaphore_signal(barrier, inc=1, device_id={"rep": z + 1}, device_id_type=MESH)

    @pl.when(z > 0)
    def _():
        pl.semaphore_signal(barrier, inc=1, device_id={"rep": z - 1}, device_id_type=MESH)

    z_near = jnp.where(z > 0, 1, 0) + jnp.where(z + 1 < reps, 1, 0)
    pl.semaphore_wait(barrier, len(near) + z_near)
    pl.semaphore_signal(far_sem, inc=1, device_id={"tp": xn}, device_id_type=MESH)

    dn_s, dn_r = take("send"), take("recv")
    up_s, up_r = take("send"), take("recv")

    def send_dn(j):
        cols = pl.ds(pl.multiple_of(j * f_own, f_own), f_own)
        remote(dn_own.at[:, cols], dn_all.at[me, dn_rows, :], "tp", j, dn_s, dn_r).start()

    def send_up(j):
        cols = pl.ds(pl.multiple_of(j * c_own, c_own), c_own)
        remote(up_own.at[:, cols], up_all.at[me, up_rows, :], "tp", j, up_s, up_r).start()

    dn_stage.wait()
    for j in near:
        send_dn(j)
    pl.semaphore_wait(far_sem, 1)
    for j in (dg, mate_of(dg)):
        send_dn(j)
    up_stage.wait()
    for j in near + (dg, mate_of(dg)):
        send_up(j)
    own_load.wait()

    def chunk(slot, b):
        return a_all.at[slot, pl.ds(b * chunk_rows, chunk_rows), :]

    x_order, y_order = link_orders(chunks)
    x_own, y_own, passed_on, x_pass, y_pass, d_pass = (take("send") for _ in range(6))
    event_r, side_r, diag_r = take("recv", len(x_order)), take("recv", blocks), take("recv", blocks)

    def issue(k):
        if k < len(x_order):
            passed, b = x_order[k]
            src = chunk(yn if passed else me, b)
            remote(src, src, "tp", xn, passed_on if passed else x_own, event_r + k).start()
            passed, b = y_order[k]
            src = chunk(xn if passed else me, b)
            remote(src, src, "tp", yn, passed_on if passed else y_own, event_r + k).start()

    issued = [0]

    def issue_up_to(k):
        while issued[0] < min(k + 1 + depth, len(x_order)):
            i = issued[0]
            (x_passed, x_b), (y_passed, y_b) = x_order[i], y_order[i]
            if x_passed and y_order.index((False, x_b)) > k:
                break
            if y_passed and x_order.index((False, y_b)) > k:
                break
            issue(i)
            issued[0] += 1

    def rows_of(many):
        return a_all.at[0, pl.ds(0, many * chunk_rows), :]

    def event(k):
        drain(recv_sem.at[event_r + k], rows_of(2))
        issue_up_to(k)
        for (passed, b), side, s in ((x_order[k], xn, x_pass), (y_order[k], yn, y_pass)):
            src = chunk(dg if passed else side, b)
            r = (diag_r if passed else side_r) + b // split
            remote(src, src, "tp", mate, d_pass if passed else s, r).start()

    mate_copy = single(a_all.at[me], a_all.at[me], "tp", mate)
    issue_up_to(-1)

    w_order = (me, mate, xn, mate_of(xn), yn, mate_of(yn), dg, mate_of(dg))
    w_k = take("local", 4)
    for i, s in enumerate(w_order):
        local(weight_ref.at[pl.ds(pl.multiple_of(s * f_own, f_own), f_own), :], w_all.at[s], w_k + i // 2)

    def w_wait(i):
        drain(local_sem.at[w_k + i], w_all.at[pl.ds(0, 2)])

    tile = 256

    def multiply(at, slots, fresh=False, final=False, unroll=False):
        @pl.loop(0, width // tile, unroll=unroll)
        def _(t):
            cols = pl.ds(pl.multiple_of(t * tile, tile), tile)
            total = None if fresh else acc[at, cols]
            for slot in slots:
                term = jnp.dot(
                    a_all[slot, at, :], w_all[slot, :, cols], preferred_element_type=jnp.float32
                )
                total = term if total is None else total + term
            if final:
                out_ref[at, cols] = total.astype(out_ref.dtype)
            else:
                acc[at, cols] = total

    def of_block(b):
        return pl.ds(b * rows, rows)

    def multiply_sides(b):
        drain(recv_sem.at[side_r + b], rows_of(2 * split))
        multiply(of_block(b), (xn, mate_of(xn), yn, mate_of(yn)))

    def wait_diagonal(b):
        drain(recv_sem.at[diag_r + b], rows_of(split))

    def multiply_diagonal(b, final=False):
        wait_diagonal(b)
        multiply(of_block(b), (dg, mate_of(dg)), final=final)

    half = rank // 2
    my_half = pl.ds(pl.multiple_of(core * half, half), half)
    mate_half = pl.ds(pl.multiple_of((1 - core) * half, half), half)

    def pages(b):
        return table_ref[index_ref[b]]

    own_pairs = blocks // 2
    mate_copy.wait_recv()
    w_wait(0)
    for s in range(own_pairs):
        multiply(pl.ds(s * 2 * rows, 2 * rows), (me, mate), fresh=True)
        if s == 0:
            own_dn.wait()
            drain(recv_sem.at[dn_r], dn_own.at[:, pl.ds(0, (n - 1) * f_own)])
            dn_z = single(dn_all.at[:, dn_rows, :], dn_all.at[:, dn_rows, :], "rep", zp)

    z_s, z_r = take("send", 2 * z_parts * (reps - 1)), take("recv", 2 * z_parts * (reps - 1))

    def up_piece(owner, right, step, h):
        pages_of = pl.ds(h * (n // z_parts), n // z_parts)
        piece = up_all.at[pages_of, quarter_of(owner), :]
        k = (step * 2 + (0 if right else 1)) * z_parts + h
        return remote(piece, piece, "rep", z + 1 if right else z - 1, z_s + k, z_r + k)

    def up_sends(right, step):
        return (z + 1 < reps) & (z >= step) if right else (z > 0) & (z + step < reps)

    def up_receives(right, step):
        return z > step if right else z + 1 + step < reps

    def up_owner(right, step):
        return z - step if right else z + step

    def up_start(step, h):
        for right in (True, False):
            @pl.when(up_sends(right, step))
            def _():
                up_piece(up_owner(right, step), right, step, h).start()

    def up_event(step, h):
        for right in (True, False):
            @pl.when(up_receives(right, step))
            def _():
                up_piece(up_owner(right, step), right, step, h).wait_recv()

        if step + 1 < reps - 1:
            up_start(step + 1, h)

    own_up.wait()
    drain(recv_sem.at[up_r], up_own.at[:, pl.ds(0, (n - 1) * c_own)])
    for h in range(z_parts):
        up_start(0, h)
    for i in range(1, 4):
        w_wait(i)

    event(0)
    event(1)
    event(2)
    multiply_sides(0)
    dn_z.wait_recv()
    for b in range(blocks):
        part[b] = lax.dot_general(
            dn_all[pages(b)],
            a_all[me, of_block(b), :],
            (((1,), (1,)), ((), ())),
            preferred_element_type=jnp.float32,
        )
    half_copy = single(part.at[:, mate_half, :], half_in, "tp", mate)
    event(3)
    event(4)
    half_copy.wait_recv()
    chip_part[...] = part[:, my_half, :] + half_in[...]
    x_out[...] = chip_part[...].astype(x_out.dtype)
    x_swap = single(x_out, x_in, "tp", xn)
    multiply_diagonal(0)
    event(5)
    up_event(0, 0)
    multiply_sides(1)
    event(6)
    multiply_diagonal(1)
    event(7)
    up_event(0, 1)
    event(8)
    multiply_sides(2)
    event(9)
    x_swap.wait_recv()
    chip_part[...] += x_in[...].astype(jnp.float32)
    y_out[...] = chip_part[...].astype(y_out.dtype)
    y_swap = single(y_out, y_in, "tp", yn)
    up_event(1, 0)
    event(10)
    multiply_diagonal(2)
    event(11)
    up_event(1, 1)
    multiply_sides(3)
    event(12)
    event(13)
    multiply_diagonal(3)
    event(14)
    multiply_sides(4)
    event(15)
    y_swap.wait_recv()
    sum_all[:, my_half, :] = (chip_part[...] + y_in[...].astype(jnp.float32)).astype(sum_all.dtype)
    sum_mate = single(sum_all.at[:, my_half, :], sum_all.at[:, my_half, :], "tp", mate)
    event(16)
    multiply_diagonal(blocks - 2)
    multiply_sides(blocks - 1)
    sum_mate.wait_recv()
    for h in range(z_parts):
        up_event(2, h)

    last = blocks - 1
    for b in range(blocks):
        at = of_block(b)
        adapted = lax.dot_general(
            sum_all[b],
            up_all[pages(b)],
            (((0,), (0,)), ((), ())),
            preferred_element_type=jnp.float32,
        )
        total = acc[at, :] + adapter_scale * adapted
        if b < last:
            out_ref[at, :] = total.astype(out_ref.dtype)
        else:
            acc[at, :] = total
    event(17)
    multiply(of_block(last), (dg,), unroll=True)
    wait_diagonal(last)
    multiply(of_block(last), (mate_of(dg),), final=True, unroll=True)

    for copy in singles:
        copy.wait_send()
    drain(send_sem.at[dn_s], dn_own.at[:, pl.ds(0, (n - 1) * f_own)])
    drain(send_sem.at[up_s], up_own.at[:, pl.ds(0, (n - 1) * c_own)])
    for s in (x_own, y_own, passed_on, x_pass, y_pass, d_pass):
        drain(send_sem.at[s], a_all.at[0])
    for step in range(reps - 1):
        for right in (True, False):
            @pl.when(up_sends(right, step))
            def _():
                for h in range(z_parts):
                    up_piece(up_owner(right, step), right, step, h).wait_send()


def shards(n, reps, attn, weight, down, up, index, table):
    tokens, f_own = attn.shape
    blocks = index.shape[0]
    rows = tokens // blocks
    features, width = weight.shape
    rank = down.shape[1]
    sends, receives = semaphore_counts(blocks, reps)
    half = (blocks, rank // 2, rows)
    return pl.pallas_call(
        functools.partial(kernel, n, reps),
        out_shape=pltpu.VMEM((tokens, width), jnp.bfloat16),
        in_specs=[pl.BlockSpec(memory_space=pltpu.SMEM)] * 2
        + [pl.BlockSpec(memory_space=pltpu.HBM)] * 4,
        out_specs=pl.BlockSpec(memory_space=pltpu.VMEM),
        scratch_shapes=[
            pltpu.VMEM((n, tokens, f_own), jnp.bfloat16),
            pltpu.VMEM((n, features // n, width), jnp.bfloat16),
            pltpu.VMEM((tokens, width), jnp.float32),
            pltpu.VMEM((rank // 2, features), jnp.bfloat16),
            pltpu.VMEM((rank // reps, n * width), jnp.bfloat16),
            pltpu.VMEM((n, rank, f_own), jnp.bfloat16),
            pltpu.VMEM((n, rank, width), jnp.bfloat16),
            pltpu.VMEM((blocks, rank, rows), jnp.float32),
            pltpu.VMEM(half, jnp.float32),
            pltpu.VMEM(half, jnp.float32),
            pltpu.VMEM(half, jnp.bfloat16),
            pltpu.VMEM(half, jnp.bfloat16),
            pltpu.VMEM(half, jnp.bfloat16),
            pltpu.VMEM(half, jnp.bfloat16),
            pltpu.VMEM((blocks, rank, rows), jnp.bfloat16),
            pltpu.SemaphoreType.DMA((sends,)),
            pltpu.SemaphoreType.DMA((receives,)),
            pltpu.SemaphoreType.DMA((9,)),
            pltpu.SemaphoreType.REGULAR,
        ],
        compiler_params=pltpu.CompilerParams(
            collective_id=0, has_side_effects=True, vmem_limit_bytes=60 * 1024 * 1024
        ),
    )(index, table, attn, weight, down, up)


def solution(mesh):
    n, reps = mesh.shape["tp"], mesh.shape["rep"]

    def body(attn, weight, down, up, index, table):
        blocks = index.shape[0]
        fits = (
            n == 8
            and reps == 4
            and blocks % 2 == 0
            and blocks == 6
            and down.shape[0] == 1
            and down.shape[1] % (16 * reps) == 0
            and down.shape[1] % (8 * n) == 0
            and attn.shape[0] % (128 * blocks) == 0
            and attn.shape[1] % 128 == 0
            and weight.shape[1] % 256 == 0
        )
        if fits:
            return shards(n, reps, attn, weight, down, up, index, table)
        return plain_shards(attn, weight, down, up, index, table)

    return jax.shard_map(
        body,
        mesh=mesh,
        in_specs=(
            P("rep", "tp"),
            P(None, "tp"),
            P("tp", None, None),
            P("tp", None, None),
            P("rep"),
            P(),
        ),
        out_specs=P("rep", "tp"),
        check_vma=False,
    )
```

```python
import functools

import jax
import jax.numpy as jnp
from jax import lax
from jax.experimental import pallas as pl
from jax.experimental.pallas import tpu as pltpu
from jax.sharding import PartitionSpec as P

adapter_scale = 2.0
MESH = pl.DeviceIdType.MESH


def plain_shards(
    attn,
    output_weight,
    adapter_down_weight,
    adapter_up_weight,
    block_adapter_index,
    adapter_page_table,
):
    tokens = attn.shape[0]
    blocks = block_adapter_index.shape[0]
    block_rows = tokens // blocks
    page_slot_count = adapter_down_weight.shape[0]
    width_out = output_weight.shape[1]
    position = lax.axis_index("tp")
    block_page_index = adapter_page_table[block_adapter_index]
    up_weight_columns = lax.all_to_all(
        adapter_up_weight, "tp", split_axis=2, concat_axis=0, tiled=True
    )
    block_up = up_weight_columns[block_page_index]
    gathered = lax.all_gather(attn, "tp", axis=1, tiled=True)
    base_output = jnp.dot(gathered, output_weight, preferred_element_type=jnp.float32)
    row_blocks = gathered.reshape(blocks, block_rows, gathered.shape[1])
    side_sum = jnp.einsum(
        "btf,srf->bsrt", row_blocks, adapter_down_weight, preferred_element_type=jnp.float32
    )
    own_pages = position * page_slot_count + jnp.arange(page_slot_count, dtype=jnp.int32)
    owned = (block_page_index[:, None] == own_pages[None, :]).astype(jnp.float32)
    local_term = jnp.sum(owned[:, :, None, None] * side_sum, axis=1)
    shrunk = lax.psum(local_term.astype(jnp.bfloat16), "tp")
    adapter_output = jnp.einsum(
        "brt,brc->btc", shrunk, block_up, preferred_element_type=jnp.float32
    )
    adapter_output = adapter_output.reshape(tokens, width_out)
    return (base_output + adapter_scale * adapter_output).astype(jnp.bfloat16)


depth = 4
split = 2
z_parts = 2


def link_orders(chunks):
    x_order, y_order = [(False, 1), (False, 0), (False, 3)], [(False, 0), (False, 1), (False, 2)]
    for s in range(chunks // 2):
        x_order.append((True, 2 * s))
        y_order.append((True, 2 * s + 1))
        for order, b in ((x_order, 2 * s + 2), (x_order, 2 * s + 5), (y_order, 2 * s + 3), (y_order, 2 * s + 4)):
            if b < chunks:
                order.append((False, b))
    x_order[-6:] = [
        (False, chunks - 1), (True, chunks - 6), (False, chunks - 4),
        (False, chunks - 2), (True, chunks - 4), (True, chunks - 2),
    ]
    y_order[-6:] = [
        (False, chunks - 2), (True, chunks - 5), (False, chunks - 3),
        (False, chunks - 1), (True, chunks - 3), (True, chunks - 1),
    ]
    return x_order, y_order


def semaphore_counts(blocks, reps):
    sends = 9 + 5 + 2 * z_parts * (reps - 1)
    receives = 3 * blocks * split // 2 + 2 * blocks + 8 + 2 * z_parts * (reps - 1)
    return sends, receives


def kernel(
    n,
    reps,
    index_ref,
    table_ref,
    attn_ref,
    weight_ref,
    down_ref,
    up_ref,
    out_ref,
    a_all,
    w_all,
    acc,
    dn_own,
    up_own,
    dn_all,
    up_all,
    part,
    half_in,
    chip_part,
    x_out,
    x_in,
    y_out,
    y_in,
    sum_all,
    send_sem,
    recv_sem,
    local_sem,
    far_sem,
):
    blocks = index_ref.shape[0]
    chunks = blocks * split
    rows = a_all.shape[1] // blocks
    chunk_rows = rows // split
    rank = dn_all.shape[1]
    f_own = a_all.shape[2]
    c_own = up_all.shape[2]
    width = acc.shape[1]
    me = lax.axis_index("tp")
    z = lax.axis_index("rep")
    core = lax.rem(me, 2)
    x_at = lax.rem(me // 2, 2)
    y_at = me // 4
    mate = me + 1 - 2 * core
    xn = me + 2 - 4 * x_at
    yn = me + 4 - 8 * y_at
    dg = xn + 4 - 8 * y_at
    zp = z + 1 - 2 * lax.rem(z, 2)

    def mate_of(d):
        return d + 1 - 2 * core

    counts = {"send": 0, "recv": 0, "local": 0}

    def take(kind, many=1):
        k = counts[kind]
        counts[kind] += many
        return k

    def remote(src, dst, axis, target, s, r):
        return pltpu.make_async_remote_copy(
            src_ref=src,
            dst_ref=dst,
            send_sem=send_sem.at[s],
            recv_sem=recv_sem.at[r],
            device_id={axis: target},
            device_id_type=MESH,
        )

    def drain(sem, ref):
        pltpu.make_async_copy(ref, ref, sem).wait()

    singles = []

    def single(src, dst, axis, target):
        copy = remote(src, dst, axis, target, take("send"), take("recv"))
        copy.start()
        singles.append(copy)
        return copy

    def local(src, dst, k=None):
        copy = pltpu.make_async_copy(src, dst, local_sem.at[take("local") if k is None else k])
        copy.start()
        return copy

    quarter = rank // reps
    pair_rank = rank // 2

    def quarter_of(at):
        return pl.ds(pl.multiple_of(at * quarter, quarter), quarter)

    up_rows = quarter_of(z)
    dn_rows = pl.ds(pl.multiple_of(lax.rem(z, 2) * pair_rank, pair_rank), pair_rank)
    own_f = pl.ds(pl.multiple_of(me * f_own, f_own), f_own)
    own_c = pl.ds(pl.multiple_of(me * c_own, c_own), c_own)

    dn_stage = local(down_ref.at[0, dn_rows, :], dn_own)
    up_stage = local(up_ref.at[0, up_rows, :], up_own)
    own_load = local(attn_ref, a_all.at[me])
    own_dn = local(down_ref.at[0, dn_rows, own_f], dn_all.at[me, dn_rows, :])
    own_up = local(up_ref.at[0, up_rows, own_c], up_all.at[me, up_rows, :])

    barrier = pltpu.get_barrier_semaphore()
    near = (xn, yn, mate_of(xn), mate_of(yn), mate)
    for d in near:
        pl.semaphore_signal(barrier, inc=1, device_id={"tp": d}, device_id_type=MESH)

    @pl.when(z + 1 < reps)
    def _():
        pl.semaphore_signal(barrier, inc=1, device_id={"rep": z + 1}, device_id_type=MESH)

    @pl.when(z > 0)
    def _():
        pl.semaphore_signal(barrier, inc=1, device_id={"rep": z - 1}, device_id_type=MESH)

    z_near = jnp.where(z > 0, 1, 0) + jnp.where(z + 1 < reps, 1, 0)
    pl.semaphore_wait(barrier, len(near) + z_near)
    pl.semaphore_signal(far_sem, inc=1, device_id={"tp": xn}, device_id_type=MESH)

    dn_s, dn_r = take("send"), take("recv")
    up_s, up_r = take("send"), take("recv")

    def send_dn(j):
        cols = pl.ds(pl.multiple_of(j * f_own, f_own), f_own)
        remote(dn_own.at[:, cols], dn_all.at[me, dn_rows, :], "tp", j, dn_s, dn_r).start()

    def send_up(j):
        cols = pl.ds(pl.multiple_of(j * c_own, c_own), c_own)
        remote(up_own.at[:, cols], up_all.at[me, up_rows, :], "tp", j, up_s, up_r).start()

    dn_stage.wait()
    for j in near:
        send_dn(j)
    pl.semaphore_wait(far_sem, 1)
    for j in (dg, mate_of(dg)):
        send_dn(j)
    up_stage.wait()
    for j in near + (dg, mate_of(dg)):
        send_up(j)
    own_load.wait()

    def chunk(slot, b):
        return a_all.at[slot, pl.ds(b * chunk_rows, chunk_rows), :]

    x_order, y_order = link_orders(chunks)
    x_own, y_own, passed_on, x_pass, y_pass, d_pass = (take("send") for _ in range(6))
    event_r, side_r, diag_r = take("recv", len(x_order)), take("recv", blocks), take("recv", blocks)

    def issue(k):
        if k < len(x_order):
            passed, b = x_order[k]
            src = chunk(yn if passed else me, b)
            remote(src, src, "tp", xn, passed_on if passed else x_own, event_r + k).start()
            passed, b = y_order[k]
            src = chunk(xn if passed else me, b)
            remote(src, src, "tp", yn, passed_on if passed else y_own, event_r + k).start()

    issued = [0]

    def issue_up_to(k):
        while issued[0] < min(k + 1 + depth, len(x_order)):
            i = issued[0]
            (x_passed, x_b), (y_passed, y_b) = x_order[i], y_order[i]
            if x_passed and y_order.index((False, x_b)) > k:
                break
            if y_passed and x_order.index((False, y_b)) > k:
                break
            issue(i)
            issued[0] += 1

    def rows_of(many):
        return a_all.at[0, pl.ds(0, many * chunk_rows), :]

    def event(k):
        drain(recv_sem.at[event_r + k], rows_of(2))
        issue_up_to(k)
        for (passed, b), side, s in ((x_order[k], xn, x_pass), (y_order[k], yn, y_pass)):
            src = chunk(dg if passed else side, b)
            r = (diag_r if passed else side_r) + b // split
            remote(src, src, "tp", mate, d_pass if passed else s, r).start()

    mate_copy = single(a_all.at[me], a_all.at[me], "tp", mate)
    issue_up_to(-1)

    w_order = (me, mate, xn, mate_of(xn), yn, mate_of(yn), dg, mate_of(dg))
    w_k = take("local", 4)
    for i, s in enumerate(w_order):
        local(weight_ref.at[pl.ds(pl.multiple_of(s * f_own, f_own), f_own), :], w_all.at[s], w_k + i // 2)

    def w_wait(i):
        drain(local_sem.at[w_k + i], w_all.at[pl.ds(0, 2)])

    tile = 256

    def multiply(at, slots, fresh=False, final=False, unroll=True):
        @pl.loop(0, width // tile, unroll=unroll)
        def _(t):
            cols = pl.ds(pl.multiple_of(t * tile, tile), tile)
            total = None if fresh else acc[at, cols]
            for slot in slots:
                term = jnp.dot(
                    a_all[slot, at, :], w_all[slot, :, cols], preferred_element_type=jnp.float32
                )
                total = term if total is None else total + term
            if final:
                out_ref[at, cols] = total.astype(out_ref.dtype)
            else:
                acc[at, cols] = total

    def of_block(b):
        return pl.ds(b * rows, rows)

    def multiply_sides(b):
        drain(recv_sem.at[side_r + b], rows_of(2 * split))
        multiply(of_block(b), (xn, mate_of(xn), yn, mate_of(yn)))

    def wait_diagonal(b):
        drain(recv_sem.at[diag_r + b], rows_of(split))

    def multiply_diagonal(b, final=False):
        wait_diagonal(b)
        multiply(of_block(b), (dg, mate_of(dg)), final=final)

    half = rank // 2
    my_half = pl.ds(pl.multiple_of(core * half, half), half)
    mate_half = pl.ds(pl.multiple_of((1 - core) * half, half), half)

    def pages(b):
        return table_ref[index_ref[b]]

    own_pairs = blocks // 2
    mate_copy.wait_recv()
    w_wait(0)
    for s in range(own_pairs):
        multiply(pl.ds(s * 2 * rows, 2 * rows), (me, mate), fresh=True)
        if s == 0:
            own_dn.wait()
            drain(recv_sem.at[dn_r], dn_own.at[:, pl.ds(0, (n - 1) * f_own)])
            dn_z = single(dn_all.at[:, dn_rows, :], dn_all.at[:, dn_rows, :], "rep", zp)

    z_s, z_r = take("send", 2 * z_parts * (reps - 1)), take("recv", 2 * z_parts * (reps - 1))

    def up_piece(owner, right, step, h):
        pages_of = pl.ds(h * (n // z_parts), n // z_parts)
        piece = up_all.at[pages_of, quarter_of(owner), :]
        k = (step * 2 + (0 if right else 1)) * z_parts + h
        return remote(piece, piece, "rep", z + 1 if right else z - 1, z_s + k, z_r + k)

    def up_sends(right, step):
        return (z + 1 < reps) & (z >= step) if right else (z > 0) & (z + step < reps)

    def up_receives(right, step):
        return z > step if right else z + 1 + step < reps

    def up_owner(right, step):
        return z - step if right else z + step

    def up_start(step, h):
        for right in (True, False):
            @pl.when(up_sends(right, step))
            def _():
                up_piece(up_owner(right, step), right, step, h).start()

    def up_event(step, h):
        for right in (True, False):
            @pl.when(up_receives(right, step))
            def _():
                up_piece(up_owner(right, step), right, step, h).wait_recv()

        if step + 1 < reps - 1:
            up_start(step + 1, h)

    own_up.wait()
    drain(recv_sem.at[up_r], up_own.at[:, pl.ds(0, (n - 1) * c_own)])
    for h in range(z_parts):
        up_start(0, h)
    for i in range(1, 4):
        w_wait(i)

    event(0)
    event(1)
    event(2)
    multiply_sides(0)
    dn_z.wait_recv()
    for b in range(blocks):
        part[b] = lax.dot_general(
            dn_all[pages(b)],
            a_all[me, of_block(b), :],
            (((1,), (1,)), ((), ())),
            preferred_element_type=jnp.float32,
        )
    half_copy = single(part.at[:, mate_half, :], half_in, "tp", mate)
    event(3)
    event(4)
    half_copy.wait_recv()
    chip_part[...] = part[:, my_half, :] + half_in[...]
    x_out[...] = chip_part[...].astype(x_out.dtype)
    x_swap = single(x_out, x_in, "tp", xn)
    multiply_diagonal(0)
    event(5)
    up_event(0, 0)
    multiply_sides(1)
    event(6)
    event(7)
    up_event(0, 1)
    multiply_diagonal(1)
    event(8)
    multiply_sides(2)
    event(9)
    x_swap.wait_recv()
    chip_part[...] += x_in[...].astype(jnp.float32)
    y_out[...] = chip_part[...].astype(y_out.dtype)
    y_swap = single(y_out, y_in, "tp", yn)
    up_event(1, 0)
    event(10)
    multiply_diagonal(2)
    event(11)
    up_event(1, 1)
    multiply_sides(3)
    event(12)
    event(13)
    event(14)
    multiply_diagonal(3)
    y_swap.wait_recv()
    sum_all[:, my_half, :] = (chip_part[...] + y_in[...].astype(jnp.float32)).astype(sum_all.dtype)
    sum_mate = single(sum_all.at[:, my_half, :], sum_all.at[:, my_half, :], "tp", mate)
    multiply_sides(blocks - 2)
    event(15)

    def add_adapted(b, final):
        at = of_block(b)
        adapted = lax.dot_general(
            sum_all[b],
            up_all[pages(b)],
            (((0,), (0,)), ((), ())),
            preferred_element_type=jnp.float32,
        )
        total = acc[at, :] + adapter_scale * adapted
        if final:
            out_ref[at, :] = total.astype(out_ref.dtype)
        else:
            acc[at, :] = total

    last = blocks - 1
    sum_mate.wait_recv()
    for h in range(z_parts):
        up_event(reps - 2, h)
    for b in range(blocks - 2):
        add_adapted(b, True)
    event(16)
    multiply_sides(last)
    event(17)
    multiply_diagonal(last - 1)
    multiply(of_block(last), (dg,), unroll=True)
    add_adapted(last - 1, True)
    add_adapted(last, False)
    wait_diagonal(last)
    multiply(of_block(last), (mate_of(dg),), final=True, unroll=True)

    for copy in singles:
        copy.wait_send()
    drain(send_sem.at[dn_s], dn_own.at[:, pl.ds(0, (n - 1) * f_own)])
    drain(send_sem.at[up_s], up_own.at[:, pl.ds(0, (n - 1) * c_own)])
    for s in (x_own, y_own, passed_on, x_pass, y_pass, d_pass):
        drain(send_sem.at[s], a_all.at[0])
    for step in range(reps - 1):
        for right in (True, False):
            @pl.when(up_sends(right, step))
            def _():
                for h in range(z_parts):
                    up_piece(up_owner(right, step), right, step, h).wait_send()


def shards(n, reps, attn, weight, down, up, index, table):
    tokens, f_own = attn.shape
    blocks = index.shape[0]
    rows = tokens // blocks
    features, width = weight.shape
    rank = down.shape[1]
    sends, receives = semaphore_counts(blocks, reps)
    half = (blocks, rank // 2, rows)
    return pl.pallas_call(
        functools.partial(kernel, n, reps),
        out_shape=pltpu.VMEM((tokens, width), jnp.bfloat16),
        in_specs=[pl.BlockSpec(memory_space=pltpu.SMEM)] * 2
        + [pl.BlockSpec(memory_space=pltpu.HBM)] * 4,
        out_specs=pl.BlockSpec(memory_space=pltpu.VMEM),
        scratch_shapes=[
            pltpu.VMEM((n, tokens, f_own), jnp.bfloat16),
            pltpu.VMEM((n, features // n, width), jnp.bfloat16),
            pltpu.VMEM((tokens, width), jnp.float32),
            pltpu.VMEM((rank // 2, features), jnp.bfloat16),
            pltpu.VMEM((rank // reps, n * width), jnp.bfloat16),
            pltpu.VMEM((n, rank, f_own), jnp.bfloat16),
            pltpu.VMEM((n, rank, width), jnp.bfloat16),
            pltpu.VMEM((blocks, rank, rows), jnp.float32),
            pltpu.VMEM(half, jnp.float32),
            pltpu.VMEM(half, jnp.float32),
            pltpu.VMEM(half, jnp.bfloat16),
            pltpu.VMEM(half, jnp.bfloat16),
            pltpu.VMEM(half, jnp.bfloat16),
            pltpu.VMEM(half, jnp.bfloat16),
            pltpu.VMEM((blocks, rank, rows), jnp.bfloat16),
            pltpu.SemaphoreType.DMA((sends,)),
            pltpu.SemaphoreType.DMA((receives,)),
            pltpu.SemaphoreType.DMA((9,)),
            pltpu.SemaphoreType.REGULAR,
        ],
        compiler_params=pltpu.CompilerParams(
            collective_id=0, has_side_effects=True, vmem_limit_bytes=60 * 1024 * 1024
        ),
    )(index, table, attn, weight, down, up)


def solution(mesh):
    n, reps = mesh.shape["tp"], mesh.shape["rep"]

    def body(attn, weight, down, up, index, table):
        blocks = index.shape[0]
        fits = (
            n == 8
            and reps == 4
            and blocks % 2 == 0
            and blocks == 6
            and down.shape[0] == 1
            and down.shape[1] % (16 * reps) == 0
            and down.shape[1] % (8 * n) == 0
            and attn.shape[0] % (128 * blocks) == 0
            and attn.shape[1] % 128 == 0
            and weight.shape[1] % 256 == 0
        )
        if fits:
            return shards(n, reps, attn, weight, down, up, index, table)
        return plain_shards(attn, weight, down, up, index, table)

    return jax.shard_map(
        body,
        mesh=mesh,
        in_specs=(
            P("rep", "tp"),
            P(None, "tp"),
            P("tp", None, None),
            P("tp", None, None),
            P("rep"),
            P(),
        ),
        out_specs=P("rep", "tp"),
        check_vma=False,
    )
```

```python
import functools

import jax
import jax.numpy as jnp
from jax import lax
from jax.experimental import pallas as pl
from jax.experimental.pallas import tpu as pltpu
from jax.sharding import PartitionSpec as P

adapter_scale = 2.0
MESH = pl.DeviceIdType.MESH


def plain_shards(
    attn,
    output_weight,
    adapter_down_weight,
    adapter_up_weight,
    block_adapter_index,
    adapter_page_table,
):
    tokens = attn.shape[0]
    blocks = block_adapter_index.shape[0]
    block_rows = tokens // blocks
    page_slot_count = adapter_down_weight.shape[0]
    width_out = output_weight.shape[1]
    position = lax.axis_index("tp")
    block_page_index = adapter_page_table[block_adapter_index]
    up_weight_columns = lax.all_to_all(
        adapter_up_weight, "tp", split_axis=2, concat_axis=0, tiled=True
    )
    block_up = up_weight_columns[block_page_index]
    gathered = lax.all_gather(attn, "tp", axis=1, tiled=True)
    base_output = jnp.dot(gathered, output_weight, preferred_element_type=jnp.float32)
    row_blocks = gathered.reshape(blocks, block_rows, gathered.shape[1])
    side_sum = jnp.einsum(
        "btf,srf->bsrt", row_blocks, adapter_down_weight, preferred_element_type=jnp.float32
    )
    own_pages = position * page_slot_count + jnp.arange(page_slot_count, dtype=jnp.int32)
    owned = (block_page_index[:, None] == own_pages[None, :]).astype(jnp.float32)
    local_term = jnp.sum(owned[:, :, None, None] * side_sum, axis=1)
    shrunk = lax.psum(local_term.astype(jnp.bfloat16), "tp")
    adapter_output = jnp.einsum(
        "brt,brc->btc", shrunk, block_up, preferred_element_type=jnp.float32
    )
    adapter_output = adapter_output.reshape(tokens, width_out)
    return (base_output + adapter_scale * adapter_output).astype(jnp.bfloat16)


depth = 4
split = 2
z_parts = 2


def link_orders(chunks):
    x_order, y_order = [(False, 1), (False, 0), (False, 3)], [(False, 0), (False, 1), (False, 2)]
    for s in range(chunks // 2):
        x_order.append((True, 2 * s))
        y_order.append((True, 2 * s + 1))
        for order, b in ((x_order, 2 * s + 2), (x_order, 2 * s + 5), (y_order, 2 * s + 3), (y_order, 2 * s + 4)):
            if b < chunks:
                order.append((False, b))
    x_order[-6:] = [
        (False, chunks - 1), (True, chunks - 6), (False, chunks - 4),
        (False, chunks - 2), (True, chunks - 4), (True, chunks - 2),
    ]
    y_order[-6:] = [
        (False, chunks - 2), (True, chunks - 5), (False, chunks - 3),
        (False, chunks - 1), (True, chunks - 3), (True, chunks - 1),
    ]
    return x_order, y_order


def semaphore_counts(blocks, reps):
    receives = 3 * blocks * split // 2 + 2 * blocks + 9 + 2 * z_parts * (reps - 1)
    return 13, receives


def kernel(
    n,
    reps,
    index_ref,
    table_ref,
    attn_ref,
    weight_ref,
    down_ref,
    up_ref,
    out_ref,
    a_all,
    w_all,
    acc,
    dn_own,
    up_own,
    dn_all,
    up_all,
    chip_part,
    x_out,
    x_in,
    y_out,
    y_in,
    sum_all,
    send_sem,
    recv_sem,
    local_sem,
    far_sem,
):
    blocks = index_ref.shape[0]
    chunks = blocks * split
    rows = a_all.shape[1] // blocks
    chunk_rows = rows // split
    half = dn_all.shape[1]
    rank = 2 * half
    f_own = a_all.shape[2]
    c_own = up_all.shape[2]
    width = acc.shape[1]
    me = lax.axis_index("tp")
    z = lax.axis_index("rep")
    core = lax.rem(me, 2)
    x_at = lax.rem(me // 2, 2)
    y_at = me // 4
    mate = me + 1 - 2 * core
    xn = me + 2 - 4 * x_at
    yn = me + 4 - 8 * y_at
    dg = xn + 4 - 8 * y_at

    def mate_of(d):
        return d + 1 - 2 * core

    counts = {"send": 0, "recv": 0, "local": 0}

    def take(kind, many=1):
        k = counts[kind]
        counts[kind] += many
        return k

    def remote(src, dst, axis, target, s, r):
        return pltpu.make_async_remote_copy(
            src_ref=src,
            dst_ref=dst,
            send_sem=send_sem.at[s],
            recv_sem=recv_sem.at[r],
            device_id={axis: target},
            device_id_type=MESH,
        )

    def drain(sem, ref):
        pltpu.make_async_copy(ref, ref, sem).wait()

    singles = []

    def single(src, dst, axis, target):
        copy = remote(src, dst, axis, target, take("send"), take("recv"))
        copy.start()
        singles.append(copy)
        return copy

    def local(src, dst, k=None):
        copy = pltpu.make_async_copy(src, dst, local_sem.at[take("local") if k is None else k])
        copy.start()
        return copy

    quarter = rank // reps
    z_bit = lax.rem(z, 2)
    zp = z + 1 - 2 * z_bit

    def quarter_of(at):
        return pl.ds(pl.multiple_of(at * quarter, quarter), quarter)

    eighth = f_own // 4
    f_part = 3 * eighth
    inner = (z == 1) | (z == 2)

    def features(first, eighths):
        return pl.ds(pl.multiple_of(first * eighth, eighth), eighths * eighth)

    brought = z // 2 * 2 + (1 - z_bit) * 3

    def quarter_from(plane):
        return dn_all.at[:, :, features((plane - 1) * 6, 2)]

    def half_of(at):
        return pl.ds(pl.multiple_of(at * half, half), half)

    def pages_of(h):
        return pl.ds(h * (n // z_parts), n // z_parts)

    my_half = half_of(core)
    up_rows = quarter_of(z)
    own_c = pl.ds(pl.multiple_of(me * c_own, c_own), c_own)

    dn_k = take("local")
    for chip in range(n // 2):
        local(down_ref.at[0, :, features(chip * 8 + brought, 3)], dn_own.at[:, features(chip * 3, 3)], dn_k)
    up_stage = local(up_ref.at[0, up_rows, :], up_own)
    own_load = local(attn_ref, a_all.at[me])
    own_dn = local(
        down_ref.at[0, my_half, features(me // 2 * 8 + brought, 3)], dn_all.at[me, :, features(brought, 3)]
    )
    own_up = local(up_ref.at[0, up_rows, own_c], up_all.at[me, up_rows, :])

    barrier = pltpu.get_barrier_semaphore()
    near = (xn, yn, mate_of(xn), mate_of(yn), mate)
    for d in near:
        pl.semaphore_signal(barrier, inc=1, device_id={"tp": d}, device_id_type=MESH)

    @pl.when(z + 1 < reps)
    def _():
        pl.semaphore_signal(barrier, inc=1, device_id={"rep": z + 1}, device_id_type=MESH)

    @pl.when(z > 0)
    def _():
        pl.semaphore_signal(barrier, inc=1, device_id={"rep": z - 1}, device_id_type=MESH)

    z_near = jnp.where(z > 0, 1, 0) + jnp.where(z + 1 < reps, 1, 0)
    pl.semaphore_wait(barrier, len(near) + z_near)
    pl.semaphore_signal(far_sem, inc=1, device_id={"tp": xn}, device_id_type=MESH)

    dn_s, dn_r = take("send"), take("recv")
    up_s, up_r = take("send"), take("recv")

    def send_dn(j):
        src = dn_own.at[half_of(lax.rem(j, 2)), features(j // 2 * 3, 3)]
        remote(src, dn_all.at[me, :, features(brought, 3)], "tp", j, dn_s, dn_r).start()

    def send_up(j):
        cols = pl.ds(pl.multiple_of(j * c_own, c_own), c_own)
        remote(up_own.at[:, cols], up_all.at[me, up_rows, :], "tp", j, up_s, up_r).start()

    drain(local_sem.at[dn_k], dn_own)
    for j in near:
        send_dn(j)
    pl.semaphore_wait(far_sem, 1)
    for j in (dg, mate_of(dg)):
        send_dn(j)
    up_stage.wait()
    for j in near + (dg, mate_of(dg)):
        send_up(j)
    own_load.wait()

    def chunk(slot, b):
        return a_all.at[slot, pl.ds(b * chunk_rows, chunk_rows), :]

    x_order, y_order = link_orders(chunks)
    link_s, mate_s = take("send"), take("send")
    event_r, side_r, diag_r = take("recv", len(x_order)), take("recv", blocks), take("recv", blocks)

    def issue(k):
        if k < len(x_order):
            passed, b = x_order[k]
            src = chunk(yn if passed else me, b)
            remote(src, src, "tp", xn, link_s, event_r + k).start()
            passed, b = y_order[k]
            src = chunk(xn if passed else me, b)
            remote(src, src, "tp", yn, link_s, event_r + k).start()

    issued = [0]

    def issue_up_to(k):
        while issued[0] < min(k + 1 + depth, len(x_order)):
            i = issued[0]
            (x_passed, x_b), (y_passed, y_b) = x_order[i], y_order[i]
            if x_passed and y_order.index((False, x_b)) > k:
                break
            if y_passed and x_order.index((False, y_b)) > k:
                break
            issue(i)
            issued[0] += 1

    def rows_of(many):
        return a_all.at[0, pl.ds(0, many * chunk_rows), :]

    def event(k):
        drain(recv_sem.at[event_r + k], rows_of(2))
        issue_up_to(k)
        for (passed, b), side in ((x_order[k], xn), (y_order[k], yn)):
            src = chunk(dg if passed else side, b)
            r = (diag_r if passed else side_r) + b // split
            remote(src, src, "tp", mate, mate_s, r).start()

    mate_copy = single(a_all.at[me], a_all.at[me], "tp", mate)
    issue_up_to(-1)

    w_order = (me, mate, xn, mate_of(xn), yn, mate_of(yn), dg, mate_of(dg))
    w_k = take("local", 4)
    for i, s in enumerate(w_order):
        local(weight_ref.at[pl.ds(pl.multiple_of(s * f_own, f_own), f_own), :], w_all.at[s], w_k + i // 2)

    def w_wait(i):
        drain(local_sem.at[w_k + i], w_all.at[pl.ds(0, 2)])

    tile = 256

    def multiply(at, slots, fresh=False, final=False, unroll=True):
        @pl.loop(0, width // tile, unroll=unroll)
        def _(t):
            cols = pl.ds(pl.multiple_of(t * tile, tile), tile)
            total = None if fresh else acc[at, cols]
            for slot in slots:
                term = jnp.dot(
                    a_all[slot, at, :], w_all[slot, :, cols], preferred_element_type=jnp.float32
                )
                total = term if total is None else total + term
            if final:
                out_ref[at, cols] = total.astype(out_ref.dtype)
            else:
                acc[at, cols] = total

    def of_block(b):
        return pl.ds(b * rows, rows)

    def multiply_sides(b):
        drain(recv_sem.at[side_r + b], rows_of(2 * split))
        multiply(of_block(b), (xn, mate_of(xn), yn, mate_of(yn)))

    def wait_diagonal(b):
        drain(recv_sem.at[diag_r + b], rows_of(split))

    def multiply_diagonal(b, final=False):
        wait_diagonal(b)
        multiply(of_block(b), (dg, mate_of(dg)), final=final)

    def pages(b):
        return table_ref[index_ref[b]]

    def line(piece_of, many):
        sems = {True: take("send"), False: take("send")}
        first = take("recv", 2 * z_parts * (reps - 1))

        def copy(right, step, h):
            piece = piece_of(z - step if right else z + step, h)
            k = first + (step * 2 + (0 if right else 1)) * z_parts + h
            return remote(piece, piece, "rep", z + 1 if right else z - 1, sems[right], k)

        def start(step, h):
            for right in (True, False):
                @pl.when((z + 1 < reps) & (z >= step) if right else (z > 0) & (z + step < reps))
                def _():
                    copy(right, step, h).start()

        def arrived(step, h):
            for right in (True, False):
                @pl.when(z > step if right else z + 1 + step < reps)
                def _():
                    copy(right, step, h).wait_recv()

            if step + 1 < reps - 1:
                start(step + 1, h)

        def finish():
            for right in (True, False):
                for sent in range(1, reps):
                    @pl.when(z == sent - 1 if right else z == reps - sent)
                    def _():
                        drain(send_sem.at[sems[right]], many(sent))

        return start, arrived, finish

    up_start, up_event, up_finish = line(
        lambda owner, h: up_all.at[pages_of(h), quarter_of(owner), :],
        lambda sent: up_all.at[:, pl.ds(0, sent * quarter), :],
    )
    dn_seven = dn_all.at[pl.ds(0, n - 1), :, pl.ds(0, f_part)]
    up_seven = up_own.at[:, pl.ds(0, (n - 1) * c_own)]

    own_pairs = blocks // 2
    mate_copy.wait_recv()
    w_wait(0)
    for s in range(own_pairs):
        multiply(pl.ds(s * 2 * rows, 2 * rows), (me, mate), fresh=True)
        if s == 0:
            own_dn.wait()
            drain(recv_sem.at[dn_r], dn_seven)
            side = dn_all.at[:, :, features(brought, 3)]
            dn_z = single(side, side, "rep", zp)
            cross_s, cross_r, onward_s, onward_r = take("send"), take("recv"), take("send"), take("recv")

            def cross(plane):
                return remote(quarter_from(plane), quarter_from(plane), "rep", 3 - z, cross_s, cross_r)

            def onward(plane):
                return remote(quarter_from(plane), quarter_from(plane), "rep", zp, onward_s, onward_r)

            @pl.when(inner)
            def _():
                cross(z).start()
    own_up.wait()
    drain(recv_sem.at[up_r], up_seven)
    for i in range(1, 4):
        w_wait(i)

    def add_adapted(b, final):
        at = of_block(b)
        adapted = lax.dot_general(
            sum_all[b],
            up_all[pages(b)],
            (((0,), (0,)), ((), ())),
            preferred_element_type=jnp.float32,
        )
        total = acc[at, :] + adapter_scale * adapted
        if final:
            out_ref[at, :] = total.astype(out_ref.dtype)
        else:
            acc[at, :] = total

    last = blocks - 1
    event(0)

    @pl.when(inner)
    def _():
        cross(3 - z).wait_recv()
        onward(3 - z).start()

    for h in range(z_parts):
        up_start(0, h)
    event(1)
    event(2)
    multiply_sides(0)
    event(3)
    dn_z.wait_recv()

    @pl.when(jnp.logical_not(inner))
    def _():
        onward(jnp.where(z == 0, 2, 1)).wait_recv()

    for b in range(blocks):
        page = pages(b)
        for s in range(2):
            term = lax.dot_general(
                dn_all[page, :, pl.ds(s * f_own, f_own)],
                a_all[me - core + s, of_block(b), :],
                (((1,), (1,)), ((), ())),
                preferred_element_type=jnp.float32,
            )
            total = term if s == 0 else total + term
        chip_part[b] = total
        x_out[b] = total.astype(x_out.dtype)
    x_swap = single(x_out, x_in, "tp", xn)
    event(4)
    multiply_diagonal(0)
    event(5)
    up_event(0, 0)
    multiply_sides(1)
    event(6)
    event(7)
    up_event(0, 1)
    multiply_diagonal(1)
    event(8)
    multiply_sides(2)
    event(9)
    x_swap.wait_recv()
    chip_part[...] += x_in[...].astype(jnp.float32)
    y_out[...] = chip_part[...].astype(y_out.dtype)
    y_swap = single(y_out, y_in, "tp", yn)
    up_event(1, 0)
    event(10)
    multiply_diagonal(2)
    event(11)
    up_event(1, 1)
    multiply_sides(3)
    event(12)
    event(13)
    event(14)
    y_swap.wait_recv()
    sum_all[:, my_half, :] = (chip_part[...] + y_in[...].astype(jnp.float32)).astype(sum_all.dtype)
    sum_mate = single(sum_all.at[:, my_half, :], sum_all.at[:, my_half, :], "tp", mate)
    multiply_diagonal(3)
    multiply_sides(blocks - 2)
    event(15)

    event(16)
    multiply_sides(last)
    event(17)
    sum_mate.wait_recv()
    for h in range(z_parts):
        up_event(reps - 2, h)
    for b in range(blocks - 2):
        add_adapted(b, True)
    multiply_diagonal(last - 1)
    multiply(of_block(last), (dg,), unroll=True)
    add_adapted(last - 1, True)
    add_adapted(last, False)
    wait_diagonal(last)
    multiply(of_block(last), (mate_of(dg),), final=True, unroll=True)

    for copy in singles:
        copy.wait_send()
    drain(send_sem.at[dn_s], dn_seven)
    drain(send_sem.at[up_s], up_seven)
    for s in (link_s, mate_s):
        drain(send_sem.at[s], a_all.at[pl.ds(0, 3)])
    up_finish()

    @pl.when(inner)
    def _():
        cross(z).wait_send()
        onward(3 - z).wait_send()


def shards(n, reps, attn, weight, down, up, index, table):
    tokens, f_own = attn.shape
    blocks = index.shape[0]
    rows = tokens // blocks
    features, width = weight.shape
    rank = down.shape[1]
    sends, receives = semaphore_counts(blocks, reps)
    half = (blocks, rank // 2, rows)
    return pl.pallas_call(
        functools.partial(kernel, n, reps),
        out_shape=pltpu.VMEM((tokens, width), jnp.bfloat16),
        in_specs=[pl.BlockSpec(memory_space=pltpu.SMEM)] * 2
        + [pl.BlockSpec(memory_space=pltpu.HBM)] * 4,
        out_specs=pl.BlockSpec(memory_space=pltpu.VMEM),
        scratch_shapes=[
            pltpu.VMEM((n, tokens, f_own), jnp.bfloat16),
            pltpu.VMEM((n, features // n, width), jnp.bfloat16),
            pltpu.VMEM((tokens, width), jnp.float32),
            pltpu.VMEM((rank, features // 8 * 3), jnp.bfloat16),
            pltpu.VMEM((rank // reps, n * width), jnp.bfloat16),
            pltpu.VMEM((n, rank // 2, 2 * f_own), jnp.bfloat16),
            pltpu.VMEM((n, rank, width), jnp.bfloat16),
            pltpu.VMEM(half, jnp.float32),
            pltpu.VMEM(half, jnp.bfloat16),
            pltpu.VMEM(half, jnp.bfloat16),
            pltpu.VMEM(half, jnp.bfloat16),
            pltpu.VMEM(half, jnp.bfloat16),
            pltpu.VMEM((blocks, rank, rows), jnp.bfloat16),
            pltpu.SemaphoreType.DMA((sends,)),
            pltpu.SemaphoreType.DMA((receives,)),
            pltpu.SemaphoreType.DMA((9,)),
            pltpu.SemaphoreType.REGULAR,
        ],
        compiler_params=pltpu.CompilerParams(
            collective_id=0, has_side_effects=True, vmem_limit_bytes=60 * 1024 * 1024
        ),
    )(index, table, attn, weight, down, up)


def solution(mesh):
    n, reps = mesh.shape["tp"], mesh.shape["rep"]

    def body(attn, weight, down, up, index, table):
        blocks = index.shape[0]
        fits = (
            n == 8
            and reps == 4
            and blocks % 2 == 0
            and blocks == 6
            and down.shape[0] == 1
            and down.shape[1] % (16 * reps) == 0
            and down.shape[1] % (8 * n) == 0
            and attn.shape[0] % (128 * blocks) == 0
            and attn.shape[1] % 512 == 0
            and weight.shape[1] % 256 == 0
        )
        if fits:
            return shards(n, reps, attn, weight, down, up, index, table)
        return plain_shards(attn, weight, down, up, index, table)

    return jax.shard_map(
        body,
        mesh=mesh,
        in_specs=(
            P("rep", "tp"),
            P(None, "tp"),
            P("tp", None, None),
            P("tp", None, None),
            P("rep"),
            P(),
        ),
        out_specs=P("rep", "tp"),
        check_vma=False,
    )
```

```python
import functools

import jax
import jax.numpy as jnp
from jax import lax
from jax.experimental import pallas as pl
from jax.experimental.pallas import tpu as pltpu
from jax.sharding import PartitionSpec as P

adapter_scale = 2.0
MESH = pl.DeviceIdType.MESH


def plain_shards(
    attn,
    output_weight,
    adapter_down_weight,
    adapter_up_weight,
    block_adapter_index,
    adapter_page_table,
):
    tokens = attn.shape[0]
    blocks = block_adapter_index.shape[0]
    block_rows = tokens // blocks
    page_slot_count = adapter_down_weight.shape[0]
    width_out = output_weight.shape[1]
    position = lax.axis_index("tp")
    block_page_index = adapter_page_table[block_adapter_index]
    up_weight_columns = lax.all_to_all(
        adapter_up_weight, "tp", split_axis=2, concat_axis=0, tiled=True
    )
    block_up = up_weight_columns[block_page_index]
    gathered = lax.all_gather(attn, "tp", axis=1, tiled=True)
    base_output = jnp.dot(gathered, output_weight, preferred_element_type=jnp.float32)
    row_blocks = gathered.reshape(blocks, block_rows, gathered.shape[1])
    side_sum = jnp.einsum(
        "btf,srf->bsrt", row_blocks, adapter_down_weight, preferred_element_type=jnp.float32
    )
    own_pages = position * page_slot_count + jnp.arange(page_slot_count, dtype=jnp.int32)
    owned = (block_page_index[:, None] == own_pages[None, :]).astype(jnp.float32)
    local_term = jnp.sum(owned[:, :, None, None] * side_sum, axis=1)
    shrunk = lax.psum(local_term.astype(jnp.bfloat16), "tp")
    adapter_output = jnp.einsum(
        "brt,brc->btc", shrunk, block_up, preferred_element_type=jnp.float32
    )
    adapter_output = adapter_output.reshape(tokens, width_out)
    return (base_output + adapter_scale * adapter_output).astype(jnp.bfloat16)


depth = 4
split = 2
z_parts = 2


def link_orders(chunks):
    x_order, y_order = [(False, 1), (False, 0), (False, 3)], [(False, 0), (False, 1), (False, 2)]
    for s in range(chunks // 2):
        x_order.append((True, 2 * s))
        y_order.append((True, 2 * s + 1))
        for order, b in ((x_order, 2 * s + 2), (x_order, 2 * s + 5), (y_order, 2 * s + 3), (y_order, 2 * s + 4)):
            if b < chunks:
                order.append((False, b))
    x_order[-6:] = [
        (False, chunks - 1), (True, chunks - 6), (False, chunks - 4),
        (False, chunks - 2), (True, chunks - 4), (True, chunks - 2),
    ]
    y_order[-6:] = [
        (False, chunks - 2), (True, chunks - 5), (False, chunks - 3),
        (False, chunks - 1), (True, chunks - 3), (True, chunks - 1),
    ]
    return x_order, y_order


def semaphore_counts(blocks, reps):
    receives = 2 * depth + 1 + 2 * blocks + 9 + 2 * z_parts * (reps - 1)
    return 13, receives


def kernel(
    n,
    reps,
    index_ref,
    table_ref,
    attn_ref,
    weight_ref,
    down_ref,
    up_ref,
    out_ref,
    a_all,
    w_all,
    acc,
    dn_own,
    up_own,
    dn_all,
    up_all,
    chip_part,
    x_out,
    x_in,
    y_out,
    y_in,
    sum_all,
    send_sem,
    recv_sem,
    local_sem,
    far_sem,
):
    blocks = index_ref.shape[0]
    chunks = blocks * split
    rows = a_all.shape[1] // blocks
    chunk_rows = rows // split
    half = dn_all.shape[1]
    rank = 2 * half
    f_own = a_all.shape[2]
    c_own = up_all.shape[2]
    width = acc.shape[1]
    me = lax.axis_index("tp")
    z = lax.axis_index("rep")
    core = lax.rem(me, 2)
    x_at = lax.rem(me // 2, 2)
    y_at = me // 4
    mate = me + 1 - 2 * core
    xn = me + 2 - 4 * x_at
    yn = me + 4 - 8 * y_at
    dg = xn + 4 - 8 * y_at

    def mate_of(d):
        return d + 1 - 2 * core

    counts = {"send": 0, "recv": 0, "local": 0}

    def take(kind, many=1):
        k = counts[kind]
        counts[kind] += many
        return k

    def remote(src, dst, axis, target, s, r):
        return pltpu.make_async_remote_copy(
            src_ref=src,
            dst_ref=dst,
            send_sem=send_sem.at[s],
            recv_sem=recv_sem.at[r],
            device_id={axis: target},
            device_id_type=MESH,
        )

    def drain(sem, ref):
        pltpu.make_async_copy(ref, ref, sem).wait()

    singles = []

    def single(src, dst, axis, target):
        copy = remote(src, dst, axis, target, take("send"), take("recv"))
        copy.start()
        singles.append(copy)
        return copy

    def local(src, dst, k=None):
        copy = pltpu.make_async_copy(src, dst, local_sem.at[take("local") if k is None else k])
        copy.start()
        return copy

    quarter = rank // reps
    z_bit = lax.rem(z, 2)
    zp = z + 1 - 2 * z_bit

    def quarter_of(at):
        return pl.ds(pl.multiple_of(at * quarter, quarter), quarter)

    eighth = f_own // 4
    f_part = 3 * eighth
    inner = (z == 1) | (z == 2)

    def features(first, eighths):
        return pl.ds(pl.multiple_of(first * eighth, eighth), eighths * eighth)

    brought = z // 2 * 2 + (1 - z_bit) * 3

    def quarter_from(plane):
        return dn_all.at[:, :, features((plane - 1) * 6, 2)]

    def half_of(at):
        return pl.ds(pl.multiple_of(at * half, half), half)

    def pages_of(h):
        return pl.ds(h * (n // z_parts), n // z_parts)

    my_half = half_of(core)
    up_rows = quarter_of(z)
    own_c = pl.ds(pl.multiple_of(me * c_own, c_own), c_own)

    dn_k = take("local")
    for chip in range(n // 2):
        local(down_ref.at[0, :, features(chip * 8 + brought, 3)], dn_own.at[:, features(chip * 3, 3)], dn_k)
    barrier = pltpu.get_barrier_semaphore()
    near = (xn, yn, mate_of(xn), mate_of(yn), mate)
    for d in near:
        pl.semaphore_signal(barrier, inc=1, device_id={"tp": d}, device_id_type=MESH)

    @pl.when(z + 1 < reps)
    def _():
        pl.semaphore_signal(barrier, inc=1, device_id={"rep": z + 1}, device_id_type=MESH)

    @pl.when(z > 0)
    def _():
        pl.semaphore_signal(barrier, inc=1, device_id={"rep": z - 1}, device_id_type=MESH)

    z_near = jnp.where(z > 0, 1, 0) + jnp.where(z + 1 < reps, 1, 0)
    pl.semaphore_wait(barrier, len(near) + z_near)
    pl.semaphore_signal(far_sem, inc=1, device_id={"tp": xn}, device_id_type=MESH)

    dn_s, dn_r = take("send"), take("recv")
    up_s, up_r = take("send"), take("recv")

    def send_dn(j):
        src = dn_own.at[half_of(lax.rem(j, 2)), features(j // 2 * 3, 3)]
        remote(src, dn_all.at[me, :, features(brought, 3)], "tp", j, dn_s, dn_r).start()

    def send_up(j):
        cols = pl.ds(pl.multiple_of(j * c_own, c_own), c_own)
        remote(up_own.at[:, cols], up_all.at[me, up_rows, :], "tp", j, up_s, up_r).start()

    drain(local_sem.at[dn_k], dn_own)
    up_stage = local(up_ref.at[0, up_rows, :], up_own)
    own_load = local(attn_ref, a_all.at[me])
    own_dn = local(
        down_ref.at[0, my_half, features(me // 2 * 8 + brought, 3)], dn_all.at[me, :, features(brought, 3)]
    )
    own_up = local(up_ref.at[0, up_rows, own_c], up_all.at[me, up_rows, :])
    for j in near:
        send_dn(j)
    pl.semaphore_wait(far_sem, 1)
    for j in (dg, mate_of(dg)):
        send_dn(j)
    up_stage.wait()
    for j in near + (dg, mate_of(dg)):
        send_up(j)
    own_load.wait()

    def chunk(slot, b):
        return a_all.at[slot, pl.ds(b * chunk_rows, chunk_rows), :]

    x_order, y_order = link_orders(chunks)
    link_s, mate_s = take("send"), take("send")
    ring = 2 * depth + 1
    event_r, side_r, diag_r = take("recv", ring), take("recv", blocks), take("recv", blocks)

    def issue(k):
        if k < len(x_order):
            passed, b = x_order[k]
            src = chunk(yn if passed else me, b)
            remote(src, src, "tp", xn, link_s, event_r + k % ring).start()
            passed, b = y_order[k]
            src = chunk(xn if passed else me, b)
            remote(src, src, "tp", yn, link_s, event_r + k % ring).start()

    issued = [0]

    def issue_up_to(k):
        while issued[0] < min(k + 1 + depth, len(x_order)):
            i = issued[0]
            (x_passed, x_b), (y_passed, y_b) = x_order[i], y_order[i]
            if x_passed and y_order.index((False, x_b)) > k:
                break
            if y_passed and x_order.index((False, y_b)) > k:
                break
            issue(i)
            issued[0] += 1

    def rows_of(many):
        return a_all.at[0, pl.ds(0, many * chunk_rows), :]

    def event(k):
        drain(recv_sem.at[event_r + k % ring], rows_of(2))
        issue_up_to(k)
        for (passed, b), side in ((x_order[k], xn), (y_order[k], yn)):
            src = chunk(dg if passed else side, b)
            r = (diag_r if passed else side_r) + b // split
            remote(src, src, "tp", mate, mate_s, r).start()

    mate_copy = single(a_all.at[me], a_all.at[me], "tp", mate)
    issue_up_to(-1)

    w_order = (me, mate, xn, mate_of(xn), yn, mate_of(yn), dg, mate_of(dg))
    w_k = take("local", 4)
    for i, s in enumerate(w_order):
        local(weight_ref.at[pl.ds(pl.multiple_of(s * f_own, f_own), f_own), :], w_all.at[s], w_k + i // 2)

    def w_wait(i):
        drain(local_sem.at[w_k + i], w_all.at[pl.ds(0, 2)])

    tile = 256

    def multiply(at, slots, fresh=False, final=False, unroll=True):
        @pl.loop(0, width // tile, unroll=unroll)
        def _(t):
            cols = pl.ds(pl.multiple_of(t * tile, tile), tile)
            total = None if fresh else acc[at, cols]
            for slot in slots:
                term = jnp.dot(
                    a_all[slot, at, :], w_all[slot, :, cols], preferred_element_type=jnp.float32
                )
                total = term if total is None else total + term
            if final:
                out_ref[at, cols] = total.astype(out_ref.dtype)
            else:
                acc[at, cols] = total

    def of_block(b):
        return pl.ds(b * rows, rows)

    def multiply_sides(b):
        drain(recv_sem.at[side_r + b], rows_of(2 * split))
        multiply(of_block(b), (xn, mate_of(xn), yn, mate_of(yn)))

    def wait_diagonal(b):
        drain(recv_sem.at[diag_r + b], rows_of(split))

    def multiply_diagonal(b, final=False):
        wait_diagonal(b)
        multiply(of_block(b), (dg, mate_of(dg)), final=final)

    def pages(b):
        return table_ref[index_ref[b]]

    def line(piece_of, many):
        sems = {True: take("send"), False: take("send")}
        first = take("recv", 2 * z_parts * (reps - 1))

        def copy(right, step, h):
            piece = piece_of(z - step if right else z + step, h)
            k = first + (step * 2 + (0 if right else 1)) * z_parts + h
            return remote(piece, piece, "rep", z + 1 if right else z - 1, sems[right], k)

        def start(step, h):
            for right in (True, False):
                @pl.when((z + 1 < reps) & (z >= step) if right else (z > 0) & (z + step < reps))
                def _():
                    copy(right, step, h).start()

        def arrived(step, h):
            for right in (True, False):
                @pl.when(z > step if right else z + 1 + step < reps)
                def _():
                    copy(right, step, h).wait_recv()

            if step + 1 < reps - 1:
                start(step + 1, h)

        def finish():
            for right in (True, False):
                for sent in range(1, reps):
                    @pl.when(z == sent - 1 if right else z == reps - sent)
                    def _():
                        drain(send_sem.at[sems[right]], many(sent))

        return start, arrived, finish

    up_start, up_event, up_finish = line(
        lambda owner, h: up_all.at[pages_of(h), quarter_of(owner), :],
        lambda sent: up_all.at[:, pl.ds(0, sent * quarter), :],
    )
    dn_seven = dn_all.at[pl.ds(0, n - 1), :, pl.ds(0, f_part)]
    up_seven = up_own.at[:, pl.ds(0, (n - 1) * c_own)]

    own_pairs = blocks // 2
    mate_copy.wait_recv()
    w_wait(0)
    for s in range(own_pairs):
        multiply(pl.ds(s * 2 * rows, 2 * rows), (me, mate), fresh=True)
        if s == 0:
            own_dn.wait()
            drain(recv_sem.at[dn_r], dn_seven)
            side = dn_all.at[:, :, features(brought, 3)]
            dn_z = single(side, side, "rep", zp)
            cross_s, cross_r, onward_s, onward_r = take("send"), take("recv"), take("send"), take("recv")

            def cross(plane):
                return remote(quarter_from(plane), quarter_from(plane), "rep", 3 - z, cross_s, cross_r)

            def onward(plane):
                return remote(quarter_from(plane), quarter_from(plane), "rep", zp, onward_s, onward_r)

            @pl.when(inner)
            def _():
                cross(z).start()
    own_up.wait()
    drain(recv_sem.at[up_r], up_seven)
    for i in range(1, 4):
        w_wait(i)

    def add_adapted(b, final):
        at = of_block(b)
        adapted = lax.dot_general(
            sum_all[b],
            up_all[pages(b)],
            (((0,), (0,)), ((), ())),
            preferred_element_type=jnp.float32,
        )
        total = acc[at, :] + adapter_scale * adapted
        if final:
            out_ref[at, :] = total.astype(out_ref.dtype)
        else:
            acc[at, :] = total

    last = blocks - 1
    event(0)

    @pl.when(inner)
    def _():
        cross(3 - z).wait_recv()
        onward(3 - z).start()

    for h in range(z_parts):
        up_start(0, h)
    event(1)
    event(2)
    multiply_sides(0)
    event(3)
    dn_z.wait_recv()

    @pl.when(jnp.logical_not(inner))
    def _():
        onward(jnp.where(z == 0, 2, 1)).wait_recv()

    for b in range(blocks):
        page = pages(b)
        for s in range(2):
            term = lax.dot_general(
                dn_all[page, :, pl.ds(s * f_own, f_own)],
                a_all[me - core + s, of_block(b), :],
                (((1,), (1,)), ((), ())),
                preferred_element_type=jnp.float32,
            )
            total = term if s == 0 else total + term
        chip_part[b] = total
        x_out[b] = total.astype(x_out.dtype)
    x_swap = single(x_out, x_in, "tp", xn)
    event(4)
    multiply_diagonal(0)
    event(5)
    up_event(0, 0)
    multiply_sides(1)
    event(6)
    event(7)
    up_event(0, 1)
    multiply_diagonal(1)
    event(8)
    multiply_sides(2)
    event(9)
    x_swap.wait_recv()
    chip_part[...] += x_in[...].astype(jnp.float32)
    y_out[...] = chip_part[...].astype(y_out.dtype)
    y_swap = single(y_out, y_in, "tp", yn)
    up_event(1, 0)
    event(10)
    multiply_diagonal(2)
    event(11)
    up_event(1, 1)
    multiply_sides(3)
    event(12)
    event(13)
    event(14)
    y_swap.wait_recv()
    sum_all[:, my_half, :] = (chip_part[...] + y_in[...].astype(jnp.float32)).astype(sum_all.dtype)
    sum_mate = single(sum_all.at[:, my_half, :], sum_all.at[:, my_half, :], "tp", mate)
    multiply_diagonal(3)
    multiply_sides(blocks - 2)
    event(15)

    event(16)
    multiply_sides(last)
    event(17)
    sum_mate.wait_recv()
    for h in range(z_parts):
        up_event(reps - 2, h)
    for b in range(blocks - 2):
        add_adapted(b, True)
    add_adapted(last, False)
    add_adapted(last - 1, False)
    multiply_diagonal(last - 1, final=True)
    multiply(of_block(last), (dg,), unroll=True)
    wait_diagonal(last)
    multiply(of_block(last), (mate_of(dg),), final=True, unroll=True)

    for copy in singles:
        copy.wait_send()
    drain(send_sem.at[dn_s], dn_seven)
    drain(send_sem.at[up_s], up_seven)
    for s in (link_s, mate_s):
        drain(send_sem.at[s], a_all.at[pl.ds(0, 3)])
    up_finish()

    @pl.when(inner)
    def _():
        cross(z).wait_send()
        onward(3 - z).wait_send()


def shards(n, reps, attn, weight, down, up, index, table):
    tokens, f_own = attn.shape
    blocks = index.shape[0]
    rows = tokens // blocks
    features, width = weight.shape
    rank = down.shape[1]
    sends, receives = semaphore_counts(blocks, reps)
    half = (blocks, rank // 2, rows)
    return pl.pallas_call(
        functools.partial(kernel, n, reps),
        out_shape=pltpu.VMEM((tokens, width), jnp.bfloat16),
        in_specs=[pl.BlockSpec(memory_space=pltpu.SMEM)] * 2
        + [pl.BlockSpec(memory_space=pltpu.HBM)] * 4,
        out_specs=pl.BlockSpec(memory_space=pltpu.VMEM),
        scratch_shapes=[
            pltpu.VMEM((n, tokens, f_own), jnp.bfloat16),
            pltpu.VMEM((n, features // n, width), jnp.bfloat16),
            pltpu.VMEM((tokens, width), jnp.float32),
            pltpu.VMEM((rank, features // 8 * 3), jnp.bfloat16),
            pltpu.VMEM((rank // reps, n * width), jnp.bfloat16),
            pltpu.VMEM((n, rank // 2, 2 * f_own), jnp.bfloat16),
            pltpu.VMEM((n, rank, width), jnp.bfloat16),
            pltpu.VMEM(half, jnp.float32),
            pltpu.VMEM(half, jnp.bfloat16),
            pltpu.VMEM(half, jnp.bfloat16),
            pltpu.VMEM(half, jnp.bfloat16),
            pltpu.VMEM(half, jnp.bfloat16),
            pltpu.VMEM((blocks, rank, rows), jnp.bfloat16),
            pltpu.SemaphoreType.DMA((sends,)),
            pltpu.SemaphoreType.DMA((receives,)),
            pltpu.SemaphoreType.DMA((9,)),
            pltpu.SemaphoreType.REGULAR,
        ],
        compiler_params=pltpu.CompilerParams(
            collective_id=0, has_side_effects=True, vmem_limit_bytes=60 * 1024 * 1024
        ),
    )(index, table, attn, weight, down, up)


def solution(mesh):
    n, reps = mesh.shape["tp"], mesh.shape["rep"]

    def body(attn, weight, down, up, index, table):
        blocks = index.shape[0]
        fits = (
            n == 8
            and reps == 4
            and blocks % 2 == 0
            and blocks == 6
            and down.shape[0] == 1
            and down.shape[1] % (16 * reps) == 0
            and down.shape[1] % (8 * n) == 0
            and attn.shape[0] % (128 * blocks) == 0
            and attn.shape[1] % 512 == 0
            and weight.shape[1] % 256 == 0
        )
        if fits:
            return shards(n, reps, attn, weight, down, up, index, table)
        return plain_shards(attn, weight, down, up, index, table)

    return jax.shard_map(
        body,
        mesh=mesh,
        in_specs=(
            P("rep", "tp"),
            P(None, "tp"),
            P("tp", None, None),
            P("tp", None, None),
            P("rep"),
            P(),
        ),
        out_specs=P("rep", "tp"),
        check_vma=False,
    )
```
